32 devices in a mesh: seq: 8 (over z, x), tensor: 4 (over y, core).
Axes of the slice: x: 2, y: 2, z: 4, core: 2. Of those that a mesh axis runs over, the one named last changes fastest.
Arguments:
- tokens: bfloat16 [4096, 2048], P('seq', 'tensor'), may hold values from -12 to 12
- attn_gain: float32 [2048], replicated, may hold values from 0.1 to 1.9
- w_query: bfloat16 [2048, 2048], P('seq', 'tensor'), as said below
- w_key: bfloat16 [2048, 512], P('seq', 'tensor'), as said below
- w_value: bfloat16 [2048, 512], P('seq', 'tensor'), may hold values from -0.125 to 0.125
- w_out: bfloat16 [2048, 2048], P('tensor', 'seq'), may hold values from -0.125 to 0.125
- mlp_gain: float32 [2048], replicated, may hold values from 0.1 to 1.9
- w_gate: bfloat16 [2048, 5632], P('seq', 'tensor'), may hold values from -0.125 to 0.125
- w_up: bfloat16 [2048, 5632], P('seq', 'tensor'), may hold values from -0.125 to 0.125
- w_down: bfloat16 [5632, 2048], P('tensor', 'seq'), may hold values from -0.078125 to 0.078125
Outputs:
- layer_out: bfloat16 [4096, 2048], P('seq', 'tensor')
The draws below stay inside these ranges and needn't reach their ends.
Inputs may be any that keep to these rules, and one draw needn't show every extreme that they name: `w_query`: entries are of order 2048 to the power -1/2. `w_key`: entries are of order 2048 to the power -1/2.
All inputs are finite; a program needn't handle non-finite values.
Results may differ from the reference program's by a relative error of at most 0.013.
Values may be sent and summed in bfloat16 or wider, within the bound.
A program may use at most 128 MiB of HBM per device.

```python
import jax
import jax.numpy as jnp
from jax import lax

D = 2048
HEADS = 16
KV_HEADS = 4
HEAD_DIM = 128
FF = 5632
WINDOW = 1024
TOK_DEV = 512
TOKENS = 4096


def draw_tokens(key, part):
    noise = jax.random.normal(jax.random.fold_in(key, 31), (TOKENS, D), jnp.float32)
    return jnp.clip(noise, -12.0, 12.0).astype(jnp.bfloat16)


def draw_w_query(key, part):
    base = jax.random.normal(jax.random.fold_in(key, 21), (D, HEADS * HEAD_DIM), jnp.float32) / jnp.sqrt(1.0 * D)
    bound = 9.0 / jnp.sqrt(1.0 * D)
    return jnp.clip(base, -bound, bound).astype(jnp.bfloat16)


def draw_w_key(key, part):
    base = jax.random.normal(jax.random.fold_in(key, 22), (D, KV_HEADS * HEAD_DIM), jnp.float32) / jnp.sqrt(1.0 * D)
    bound = 9.0 / jnp.sqrt(1.0 * D)
    return jnp.clip(base, -bound, bound).astype(jnp.bfloat16)


def level_of(rng, extent, pieces, smallest, largest):
    level = 1.0
    for axis_at, shards_of in pieces:
        draws = jax.random.uniform(jax.random.fold_in(jax.random.fold_in(rng, 6), axis_at), (shards_of,), jnp.float32, smallest / len(pieces), largest / len(pieces))
        level = level * jnp.repeat(jnp.exp(draws), extent[axis_at] // shards_of).reshape((-1,) + (1,) * (len(extent) - 1 - axis_at))
    return level


def scatter_about(rng, shape, width, most, shards=(), kind=jnp.bfloat16):
    result = width * jax.random.normal(rng, shape, jnp.float32)
    if shards:
        result = result * level_of(rng, shape, shards, -0.22, 0.18)
    return jnp.clip(result, -most, most).astype(kind)


def setup_inputs(seed: int = 0) -> dict:
    arg_keys = jax.random.split(jax.random.key(seed), 11)
    return {
        "tokens": draw_tokens(jax.random.fold_in(arg_keys[10], 71), 0),
        "attn_gain": jnp.clip(1.0 + 0.18 * jax.random.normal(arg_keys[1], (D,), jnp.float32), 0.1, 1.9),
        "w_query": draw_w_query(jax.random.fold_in(arg_keys[10], 71), 0),
        "w_key": draw_w_key(jax.random.fold_in(arg_keys[10], 71), 0),
        "w_value": scatter_about(arg_keys[4], (D, KV_HEADS * HEAD_DIM), D ** -0.5, 0.125, ((0, 8), (1, 4))),
        "w_out": scatter_about(arg_keys[5], (HEADS * HEAD_DIM, D), (HEADS * HEAD_DIM) ** -0.5, 0.125, ((0, 4), (1, 8))),
        "mlp_gain": jnp.clip(1.0 + 0.18 * jax.random.normal(arg_keys[6], (D,), jnp.float32), 0.1, 1.9),
        "w_gate": scatter_about(arg_keys[7], (D, FF), D ** -0.5, 0.125, ((0, 8), (1, 4))),
        "w_up": scatter_about(arg_keys[8], (D, FF), D ** -0.5, 0.125, ((0, 8), (1, 4))),
        "w_down": scatter_about(arg_keys[9], (FF, D), FF ** -0.5, 0.078125, ((0, 4), (1, 8))),
    }


def scaled_rows(values, gain):
    values = values.astype(jnp.float32)
    mean_square = lax.optimization_barrier(jnp.mean(values * values, axis=1, keepdims=True))
    return (values * lax.rsqrt(mean_square + 1e-06) * gain.astype(jnp.float32)).astype(jnp.bfloat16)

def reference(tokens, attn_gain, w_query, w_key, w_value, w_out, mlp_gain, w_gate, w_up, w_down):
    normed = scaled_rows(tokens, attn_gain)
    queries = jnp.dot(normed, w_query, preferred_element_type=jnp.float32).astype(jnp.bfloat16)
    keys = jnp.dot(normed, w_key, preferred_element_type=jnp.float32).astype(jnp.bfloat16)
    values = jnp.dot(normed, w_value, preferred_element_type=jnp.float32).astype(jnp.bfloat16)
    group = HEADS // KV_HEADS
    block = min(512, TOK_DEV)
    count = TOKENS // block
    span = WINDOW + block
    scale = HEAD_DIM ** (-0.5)
    grouped = queries.reshape(TOKENS, KV_HEADS, group, HEAD_DIM)
    padding = jnp.zeros((WINDOW, KV_HEADS * HEAD_DIM), keys.dtype)
    keys_padded = jnp.concatenate([padding, keys], axis=0)
    values_padded = jnp.concatenate([padding, values], axis=0)

    def one_block(index):
        start = (index * block).astype(jnp.int32)
        query_block = lax.dynamic_slice_in_dim(grouped, start, block, 0)
        key_block = lax.dynamic_slice_in_dim(keys_padded, start, span, 0).reshape(span, KV_HEADS, HEAD_DIM)
        value_block = lax.dynamic_slice_in_dim(values_padded, start, span, 0).reshape(span, KV_HEADS, HEAD_DIM)
        scores = jnp.einsum('qkgd,ckd->kgqc', query_block.astype(jnp.float32), key_block.astype(jnp.float32)) * scale
        query_pos = lax.broadcasted_iota(jnp.int32, (block, span), 0)
        key_pos = lax.broadcasted_iota(jnp.int32, (block, span), 1)
        distance = query_pos + WINDOW - key_pos
        allowed = (distance >= 0) & (distance < WINDOW) & (key_pos + start - WINDOW >= 0)
        scores = jnp.where(allowed[None, None], scores, -1e+30)
        highest = lax.optimization_barrier(jnp.max(scores, axis=3, keepdims=True))
        raised = jnp.exp(scores - highest)
        weights = (raised / lax.optimization_barrier(jnp.sum(raised, axis=3, keepdims=True))).astype(jnp.bfloat16)
        mixed = jnp.einsum('kgqc,ckd->qkgd', weights.astype(jnp.float32), value_block.astype(jnp.float32))
        return mixed.astype(jnp.bfloat16).reshape(block, HEADS * HEAD_DIM)
    attended = lax.map(one_block, jnp.arange(count, dtype=jnp.int32)).reshape(TOKENS, HEADS * HEAD_DIM)
    group_width = group * HEAD_DIM
    attn_sum = jnp.zeros((TOKENS, D), jnp.float32)
    for head_group in range(KV_HEADS):
        lower = head_group * group_width
        term = jnp.dot(attended[:, lower:lower + group_width], w_out[lower:lower + group_width], preferred_element_type=jnp.float32)
        term = lax.optimization_barrier(term.astype(jnp.bfloat16))
        attn_sum = attn_sum + term.astype(jnp.float32)
    stream = (tokens.astype(jnp.float32) + attn_sum).astype(jnp.bfloat16)
    stream_normed = scaled_rows(stream, mlp_gain)
    gate = jnp.dot(stream_normed, w_gate, preferred_element_type=jnp.float32)
    upward = jnp.dot(stream_normed, w_up, preferred_element_type=jnp.float32)
    hidden = (jax.nn.silu(gate) * upward).astype(jnp.bfloat16)
    block_width = FF // KV_HEADS
    mlp_sum = jnp.zeros((TOKENS, D), jnp.float32)
    for unit_block in range(KV_HEADS):
        lower = unit_block * block_width
        term = jnp.dot(hidden[:, lower:lower + block_width], w_down[lower:lower + block_width], preferred_element_type=jnp.float32)
        term = lax.optimization_barrier(term.astype(jnp.bfloat16))
        mlp_sum = mlp_sum + term.astype(jnp.float32)
    return (stream.astype(jnp.float32) + mlp_sum).astype(jnp.bfloat16)
```

```python
import functools

import jax
import jax.numpy as jnp
from jax import lax
from jax.experimental import pallas as pl
from jax.experimental.pallas import tpu as pltpu
from jax.sharding import Mesh, PartitionSpec as P

HEAD_DIM = 128
WINDOW = 1024


def product(left, right):
    return jnp.dot(left, right, preferred_element_type=jnp.float32)


def traded(block, cut):
    member = lax.axis_index("pair")
    half = block.shape[cut] // 2
    kept = lax.dynamic_slice_in_dim(block, member * half, half, cut)
    given = lax.dynamic_slice_in_dim(block, (1 - member) * half, half, cut)
    got = lax.ppermute(given, "pair", [(0, 1), (1, 0)])
    first = member == 0
    return jnp.concatenate(
        [jnp.where(first, kept, got), jnp.where(first, got, kept)], axis=1 - cut
    )


def attend(queries, keys, values, first_key):
    rows = queries.shape[0]
    span = keys.shape[0]
    group = queries.shape[1] // HEAD_DIM
    block = queries.reshape(rows, group, HEAD_DIM)
    scores = jnp.einsum("qgd,cd->gqc", block, keys, preferred_element_type=jnp.float32)
    scores = scores * HEAD_DIM ** (-0.5)
    query_pos = lax.broadcasted_iota(jnp.int32, (rows, span), 0)
    key_pos = lax.broadcasted_iota(jnp.int32, (rows, span), 1)
    distance = query_pos + WINDOW - key_pos
    allowed = (distance >= 0) & (distance < WINDOW) & (key_pos + first_key >= 0)
    scores = jnp.where(allowed[None], scores, -1e30)
    highest = jnp.max(scores, axis=2, keepdims=True)
    raised = jnp.exp(scores - highest)
    weights = (raised / jnp.sum(raised, axis=2, keepdims=True)).astype(jnp.bfloat16)
    mixed = jnp.einsum("gqc,cd->qgd", weights, values, preferred_element_type=jnp.float32)
    return mixed.astype(jnp.bfloat16).reshape(rows, group * HEAD_DIM)


def places(chips):
    member, at = lax.axis_index("pair"), lax.axis_index("tensor")
    sibling = at + 1 - 2 * lax.rem(at, 2)

    def ahead(k, start):
        return lax.rem(member + k // chips, 2), lax.rem(start + 2 * (k % chips), 2 * chips)

    def behind(k, start):
        turn = 2 * chips - 2 * (k % chips)
        return lax.rem(member + k // chips, 2), lax.rem(start + turn, 2 * chips)

    return member, at, sibling, ahead, behind


def greet(chips, at, sibling, ahead, member):
    barrier = pltpu.get_barrier_semaphore()
    for k in range(1, 2 * chips):
        there = ahead(k, at)
        pl.semaphore_signal(barrier, inc=1, device_id={"pair": there[0], "tensor": there[1]})
    pl.semaphore_signal(barrier, inc=1, device_id={"pair": member, "tensor": sibling})
    pl.semaphore_wait(barrier, 2 * chips)


def sent(source, target, send, recv, where):
    return pltpu.make_async_remote_copy(
        src_ref=source,
        dst_ref=target,
        send_sem=send,
        recv_sem=recv,
        device_id={"pair": where[0], "tensor": where[1]},
    )


def gather_kernel(chips, x_ref, gain_ref, out_ref, held, own, send, recv, pass_send, pass_recv):
    rows, cols = x_ref.shape
    member, at, sibling, ahead, behind = places(chips)

    def block(where):
        return held.at[
            pl.ds(pl.multiple_of(where[0] * rows, rows), rows),
            pl.ds(pl.multiple_of(where[1] * cols, cols), cols),
        ]

    greet(chips, at, sibling, ahead, member)
    count = 2 * chips
    mine = block((member, at))
    copies = [
        sent(x_ref, mine, send.at[k], recv.at[k], ahead(k, at)) for k in range(1, count)
    ]
    for copy in reversed(copies):
        copy.start()
    passed = [sent(x_ref, mine, pass_send.at[0], pass_recv.at[0], (member, sibling))]
    passed[0].start()
    local = pltpu.make_async_copy(x_ref, mine, own)
    local.start()
    for k in range(1, count):
        came = block(behind(k, at))
        sent(came, came, send.at[k], recv.at[k], (member, sibling)).wait_recv()
        onward = sent(came, came, pass_send.at[k], pass_recv.at[k], (member, sibling))
        onward.start()
        passed.append(onward)
    local.wait()
    for k in range(count):
        came = block(behind(k, sibling))
        sent(came, came, pass_send.at[k], pass_recv.at[k], (member, sibling)).wait_recv()
    for copy in copies + passed:
        copy.wait_send()

    step = 32

    @pl.loop(0, 2 * rows // step)
    def _(index):
        at_rows = pl.ds(pl.multiple_of(index * step, step), step)
        values = held[at_rows, :].astype(jnp.float32)
        mean_square = jnp.mean(values * values, axis=1, keepdims=True)
        scaled = values * lax.rsqrt(mean_square + 1e-06) * gain_ref[...]
        out_ref[at_rows, :] = scaled.astype(out_ref.dtype)


def normed_rows(share, gain, chips, identity):
    rows, cols = share.shape
    count = 2 * chips
    size = (2 * rows, count * cols)
    vmem = pl.BlockSpec(memory_space=pltpu.VMEM)
    return pl.pallas_call(
        functools.partial(gather_kernel, chips),
        out_shape=jax.ShapeDtypeStruct(size, jnp.bfloat16),
        in_specs=[vmem] * 2,
        out_specs=vmem,
        scratch_shapes=[
            pltpu.VMEM(size, jnp.bfloat16),
            pltpu.SemaphoreType.DMA,
            pltpu.SemaphoreType.DMA((count,)),
            pltpu.SemaphoreType.DMA((count,)),
            pltpu.SemaphoreType.DMA((count,)),
            pltpu.SemaphoreType.DMA((count,)),
        ],
        cost_estimate=pl.CostEstimate(
            flops=60 * size[0] * size[1], bytes_accessed=20 * size[0] * size[1], transcendentals=0
        ),
        compiler_params=pltpu.CompilerParams(collective_id=identity, has_side_effects=True),
    )(share, gain.reshape(1, -1))


def sum_kernel(
    chips, terms, base, out_ref, near, stage, far, near_send, near_recv, send, recv
):
    rows, cols = base.shape
    member, at, sibling, ahead, behind = places(chips)
    count = 2 * chips

    def block(where):
        return terms.at[
            pl.ds(pl.multiple_of(where[0] * rows, rows), rows),
            pl.ds(pl.multiple_of(where[1] * cols, cols), cols),
        ]

    greet(chips, at, sibling, ahead, member)
    order = list(range(count - 1, -1, -1))
    given = {
        k: sent(
            block(ahead(k, sibling)),
            near.at[k],
            near_send.at[k],
            near_recv.at[k],
            (member, sibling),
        )
        for k in order
    }
    for k in order:
        given[k].start()
    step = 64
    copies = {}
    for k in order:
        given[k].wait_recv()
        own = block(ahead(k, at))

        @pl.loop(0, rows // step)
        def _(index, k=k, own=own):
            part = pl.ds(pl.multiple_of(index * step, step), step)
            total = own[part, :].astype(jnp.float32) + near[k, part, :].astype(jnp.float32)
            stage[k, part, :] = total.astype(jnp.bfloat16)

        if k:
            copies[k] = sent(stage.at[k], far.at[k], send.at[k], recv.at[k], ahead(k, at))
            copies[k].start()
    for k in order[:-1]:
        copies[k].wait_recv()

    @pl.loop(0, rows // step)
    def _(index):
        part = pl.ds(pl.multiple_of(index * step, step), step)
        total = stage[0, part, :].astype(jnp.float32)
        for k in range(1, count):
            total = total + far[k, part, :].astype(jnp.float32)
        out_ref[part, :] = (base[part, :].astype(jnp.float32) + total).astype(out_ref.dtype)

    for k in order:
        given[k].wait_send()
        if k:
            copies[k].wait_send()


def added_share(terms, base, chips, identity):
    rows, cols = base.shape
    count = 2 * chips
    vmem = pl.BlockSpec(memory_space=pltpu.VMEM)
    slots = pltpu.VMEM((count, rows, cols), jnp.bfloat16)
    return pl.pallas_call(
        functools.partial(sum_kernel, chips),
        out_shape=jax.ShapeDtypeStruct(base.shape, jnp.bfloat16),
        in_specs=[vmem] * 2,
        out_specs=vmem,
        scratch_shapes=[slots] * 3 + [pltpu.SemaphoreType.DMA((count,))] * 4,
        cost_estimate=pl.CostEstimate(
            flops=60 * terms.size, bytes_accessed=20 * terms.size, transcendentals=0
        ),
        compiler_params=pltpu.CompilerParams(collective_id=identity, has_side_effects=True),
    )(terms, base)


def per_device(tokens, attn_gain, w_query, w_key, w_value, w_out, mlp_gain, w_gate, w_up, w_down):
    rows = tokens.shape[0]
    hi, member = lax.axis_index("hi"), lax.axis_index("pair")
    runs = lax.axis_size("hi")
    swap = [(0, 1), (1, 0)]
    first = member == 0
    kept = jnp.where(first, w_key, w_value)
    got = lax.ppermute(jnp.where(first, w_value, w_key), "pair", swap)
    pair_rows = [jnp.where(first, kept, got), jnp.where(first, got, kept)]
    kv_rows = jnp.concatenate(pair_rows, axis=0)
    qkv = jnp.concatenate([traded(w_query, 1), kv_rows], axis=1)
    qkv_full = lax.all_gather(qkv, "hi", axis=0, tiled=True)
    out_full = lax.all_gather(traded(w_out, 0), "hi", axis=1, tiled=True)
    gate_up = jnp.concatenate([traded(w_gate, 1), traded(w_up, 1)], axis=1)
    gate_up_full = lax.all_gather(gate_up, "hi", axis=0, tiled=True)
    down_full = lax.all_gather(traded(w_down, 0), "hi", axis=1, tiled=True)

    chips = lax.axis_size("tensor") // 2
    normed = normed_rows(tokens, attn_gain, chips, 1)
    width = w_query.shape[1] // 2
    projected = product(normed, qkv_full).astype(jnp.bfloat16)
    queries, mine = projected[:, :width], projected[:, width:]
    other = lax.ppermute(mine, "pair", swap)
    onward = [(i, i + 1) for i in range(runs - 1)]
    across = [
        (i * 2 + m, (i + 1) * 2 + 1 - m) for i in range(runs - 1) for m in range(2)
    ]
    mine_before = lax.ppermute(mine, "hi", onward)
    other_before = lax.ppermute(mine, ("hi", "pair"), across)
    mine = jnp.concatenate([mine_before, mine], axis=0)
    other = jnp.concatenate([other_before, other], axis=0)
    keys = jnp.where(first, mine, other)
    values = jnp.where(first, other, mine)
    blocks = []
    before = 2 * rows
    for at in range(0, 2 * rows, rows):
        start = before + at - WINDOW
        stop = before + at + rows
        blocks.append(
            attend(
                queries[at : at + rows],
                keys[start:stop],
                values[start:stop],
                (hi - 1) * before + start,
            )
        )
    attended = jnp.concatenate(blocks, axis=0)
    attn_terms = product(attended, out_full).astype(jnp.bfloat16)
    stream = added_share(attn_terms, tokens, chips, 2)
    stream_normed = normed_rows(stream, mlp_gain, chips, 3)
    units = gate_up_full.shape[1] // 2
    gate_upward = product(stream_normed, gate_up_full)
    gate, upward = gate_upward[:, :units], gate_upward[:, units:]
    hidden = (jax.nn.silu(gate) * upward).astype(jnp.bfloat16)
    return added_share(product(hidden, down_full).astype(jnp.bfloat16), stream, chips, 4)


def solution(mesh):
    sizes = mesh.shape
    split = Mesh(
        mesh.devices.reshape(sizes["seq"] // 2, 2, sizes["tensor"]), ("hi", "pair", "tensor")
    )
    seq = ("hi", "pair")
    in_specs = (
        P(seq, "tensor"),
        P(),
        P(seq, "tensor"),
        P(seq, "tensor"),
        P(seq, "tensor"),
        P("tensor", seq),
        P(),
        P(seq, "tensor"),
        P(seq, "tensor"),
        P("tensor", seq),
    )
    return jax.shard_map(
        per_device, mesh=split, in_specs=in_specs, out_specs=P(seq, "tensor"), check_vma=False
    )
```
